256 devices in a mesh: rows: 32 (over x, z), grp: 8 (over y, core).
Axes of the slice: x: 4, y: 4, z: 8, core: 2. Of those that a mesh axis runs over, the one named last changes fastest.
Arguments:
- matrix: float32 [524288, 1024], P(('rows', 'grp'))
- row_signs: int32 [524288], P(('rows', 'grp')), may hold values from -1 to 1, as said below
- samples: int32 [8192], P(('rows', 'grp')), may hold values from 0 to 524287, as said below
Outputs:
- factor: float32 [1024, 1024], P('rows')
The draws below stay inside these ranges and needn't reach their ends.
Inputs may be any that keep to these rules, and one draw needn't show every extreme that they name: `row_signs`: every entry is 1 or -1. `samples`: entries are distinct and increasing; entries k * 32 to (k + 1) * 32 - 1 lie in rows k * 2048 to (k + 1) * 2048 - 1.
All inputs are finite; a program needn't handle non-finite values.
Results may differ from the reference program's by a relative error of at most 0.00011.
Values sent between devices are 32-bit elements; how exact they have to be, the bound alone decides.
No kernel may reach another device: no remote copies, remote signals or barrier semaphores. Data moves between devices by JAX's collectives and lax.ppermute only.
A program may use at most 128 MiB of HBM per device.

```python
import jax
import jax.numpy as jnp
from jax import lax

COLS = 1024
ROW_DEV = 2048
SAMPLES = 8192
ROWS_TOTAL = 524288


def draw_matrix(key, part):
    key_noise = jax.random.fold_in(key, 11)
    key_common = jax.random.fold_in(key, 12)
    key_cols = jax.random.fold_in(key, 13)
    col_scale = jnp.exp(jax.random.uniform(key_cols, (COLS,), jnp.float32, jnp.log(0.5), jnp.log(4.0)))
    noise = jax.random.normal(key_noise, (ROWS_TOTAL, COLS), jnp.float32)
    common = jax.random.normal(key_common, (ROWS_TOTAL, 1), jnp.float32)
    mixed_rows = noise + 0.5 * jnp.roll(noise, 1, axis=1) + 0.6 * common
    return (mixed_rows * col_scale[None, :] / jnp.sqrt(jnp.float32(ROWS_TOTAL))).astype(jnp.float32)


def draw_row_signs(key, part):
    coin_key = jax.random.fold_in(key, 21)
    return (2 * jax.random.randint(coin_key, (ROWS_TOTAL,), 0, 2) - 1).astype(jnp.int32)


def draw_samples(key, part):
    pick_key = jax.random.fold_in(key, 31)
    block_count = ROWS_TOTAL // ROW_DEV
    per_block = SAMPLES // block_count
    block_keys = jax.random.split(pick_key, block_count)
    picks = jax.vmap(lambda one_key: jnp.sort(jax.random.permutation(one_key, ROW_DEV)[:per_block]))(block_keys)
    offsets = ROW_DEV * jnp.arange(block_count, dtype=jnp.int32)[:, None]
    return (picks.astype(jnp.int32) + offsets).reshape(block_count * per_block).astype(jnp.int32)


def setup_inputs(seed: int = 0) -> dict:
    keys = jax.random.split(jax.random.key(seed), 4)
    return {
        "matrix": draw_matrix(jax.random.fold_in(keys[3], 71), 0),
        "row_signs": draw_row_signs(jax.random.fold_in(keys[3], 71), 0),
        "samples": draw_samples(jax.random.fold_in(keys[3], 71), 0),
    }


def walsh_transform(values):
    length, width_cols = values.shape
    half_span = 1
    for section_level in range(length.bit_length() - 1):
        paired = values.reshape(length // (2 * half_span), 2, half_span, width_cols)
        values = jnp.stack([paired[:, 0] + paired[:, 1], paired[:, 0] - paired[:, 1]], axis=1).reshape(length, width_cols)
        half_span = half_span * 2
    return values

def reference(matrix, row_signs, samples):
    total_rows = matrix.shape[0]
    signed = matrix * row_signs.astype(jnp.float32)[:, None]
    transformed = walsh_transform(signed) / jnp.sqrt(jnp.float32(total_rows))
    sampled = transformed[samples] * jnp.sqrt(jnp.float32(total_rows / SAMPLES))
    gram_total = jnp.dot(sampled.T, sampled, precision=lax.Precision.HIGHEST)
    lower_factor = jnp.linalg.cholesky(gram_total)
    return lower_factor.T
```

```python
import functools

import jax
import jax.numpy as jnp
from jax import lax
from jax.experimental import pallas as pl
from jax.experimental.pallas import tpu as pltpu
from jax.sharding import Mesh
from jax.sharding import PartitionSpec as P

ALL = ("x", "z", "y", "c")
PLANE = ("y", "c", "x")
EXACT = lax.Precision.HIGHEST
F32 = jnp.float32
BF16 = jnp.bfloat16
COLS = 1024
BLOCKS = 256
TILE = 128


def vmem(limit=100):
    return pltpu.CompilerParams(vmem_limit_bytes=limit * 1024 * 1024 // 2)


def turn_kernel(sign_ref, in_ref, out_ref):
    for t in range(in_ref.shape[0] // TILE):
        rows = slice(t * TILE, (t + 1) * TILE)
        sign = sign_ref[t : t + 1, :].astype(F32)
        out_ref[:, rows] = in_ref[rows, :].T * sign


def turned(matrix, row_signs):
    rows, cols = matrix.shape
    signs = row_signs.reshape(rows // TILE, TILE)
    return pl.pallas_call(
        turn_kernel,
        grid=(cols // TILE,),
        in_specs=[
            pl.BlockSpec(signs.shape, lambda i: (0, 0)),
            pl.BlockSpec((rows, TILE), lambda i: (0, i)),
        ],
        out_specs=pl.BlockSpec((TILE, rows), lambda i: (i, 0)),
        out_shape=jax.ShapeDtypeStruct((cols, rows), F32),
        compiler_params=vmem(),
        name="turn",
    )(signs, matrix)


def odd_ones(bits, count):
    for shift in (8, 4, 2, 1):
        if shift < count:
            bits = bits ^ (bits >> shift)
    return bits & 1


def signs_kernel(z_ref, sample_ref, low_ref, high_ref):
    block = pl.program_id(0)
    within = sample_ref[pl.ds(block, 1), :] & 2047
    wl = lax.broadcasted_iota(jnp.int32, (256, 256), 0)
    low = odd_ones(wl & (within & 255), 8)
    low_ref[0] = (1 - 2 * low).astype(F32).astype(BF16)
    wh = lax.broadcasted_iota(jnp.int32, (8, 256), 0)
    lane = lax.broadcasted_iota(jnp.int32, (8, 256), 1)
    odd = odd_ones(wh & (within >> 8), 4) ^ odd_ones((lane >> 5) & z_ref[0], 4)
    high_ref[0] = (1 - 2 * odd).astype(F32) * (2.0**-7)


def sampled_signs(z_index, samples):
    return pl.pallas_call(
        signs_kernel,
        grid=(32,),
        in_specs=[
            pl.BlockSpec(memory_space=pltpu.SMEM),
            pl.BlockSpec((32, 256), lambda i: (0, 0)),
        ],
        out_specs=[
            pl.BlockSpec((1, 256, 256), lambda i: (i, 0, 0)),
            pl.BlockSpec((1, 8, 256), lambda i: (i, 0, 0)),
        ],
        out_shape=[
            jax.ShapeDtypeStruct((32, 256, 256), BF16),
            jax.ShapeDtypeStruct((32, 8, 256), F32),
        ],
        compiler_params=vmem(),
        name="signs",
    )(z_index, samples)


def butterflies(values):
    span = 1
    while span < len(values):
        new = list(values)
        for i in range(len(values)):
            if not i & span:
                new[i] = values[i] + values[i + span]
                new[i + span] = values[i] - values[i + span]
        values = new
        span *= 2
    return values


def pick_kernel(in_ref, low_ref, high_ref, out_ref, parts_ref):
    wh = pl.program_id(0)

    @pl.when(wh == 0)
    def _():
        out_ref[...] = jnp.zeros_like(out_ref)

    for row in range(0, 32, 16):
        for lane in range(0, 256, TILE):
            lanes = slice(lane, lane + TILE)
            values = butterflies([in_ref[p, row : row + 16, lanes] for p in range(32)])
            for p in range(32):
                rest = values[p]
                for part in range(3):
                    piece = rest.astype(BF16)
                    parts_ref[p, 32 * part + row : 32 * part + row + 16, lanes] = piece
                    if part < 2:
                        rest = rest - piece.astype(F32)

    def one(p, carry):
        got = jnp.dot(parts_ref[p], low_ref[p], preferred_element_type=F32)
        got = got[0:32] + got[32:64] + got[64:96]
        out_ref[p] = out_ref[p] + got * high_ref[p, pl.ds(wh, 1), :]
        return carry

    lax.fori_loop(0, 32, one, 0, unroll=4)


def picked(blocks, low, high):
    return pl.pallas_call(
        pick_kernel,
        grid=(8,),
        in_specs=[
            pl.BlockSpec((32, 32, 256), lambda i: (0, 0, i)),
            pl.BlockSpec((32, 256, 256), lambda i: (0, 0, 0)),
            pl.BlockSpec((32, 8, 256), lambda i: (0, 0, 0)),
        ],
        out_specs=pl.BlockSpec((32, 32, 256), lambda i: (0, 0, 0)),
        out_shape=jax.ShapeDtypeStruct((32, 32, 256), F32),
        scratch_shapes=[pltpu.VMEM((32, 96, 256), BF16)],
        compiler_params=vmem(),
        name="pick",
    )(blocks, low, high)


def gram_kernel(own_ref, near_ref, far_ref, o_own_ref, o_near_ref, o_far_ref, out_ref):
    others = (own_ref, o_own_ref, near_ref, o_near_ref, far_ref, o_far_ref)
    for tile, other in enumerate(others):
        out_ref[tile] = lax.dot_general(
            own_ref[...],
            other[...],
            (((1,), (1,)), ((), ())),
            precision=EXACT,
            preferred_element_type=F32,
        )


def gram_tiles(*blocks):
    return pl.pallas_call(
        gram_kernel,
        out_shape=jax.ShapeDtypeStruct((6, TILE, TILE), F32),
        compiler_params=vmem(),
        name="gram",
    )(*blocks)


def over_lanes(block, lane):
    return jnp.broadcast_to(block[:, lane : lane + 1], (8, TILE))


def over_rows(block, row):
    return jnp.broadcast_to(block[row : row + 1, :], (8, TILE))


def inverse_root(d):
    root = lax.rsqrt(d)
    return root * (1.5 - 0.5 * (d * root) * root)


def factor_kernel(at_ref, *refs):
    tile_refs = refs[:8]
    out_ref, work, left = refs[8:]
    y, c, row0 = at_ref[0], at_ref[1], at_ref[2]
    for n, ref in enumerate(tile_refs):
        shift, other = n % 4, n // 4
        ys, cs = (y + shift) % 4, c ^ other
        a = 2 * ys + cs
        for tile in range(ref.shape[0]):
            dy, dc = tile // 2, tile % 2
            b = 2 * ((ys + dy) % 4) + (cs ^ dc)

            @pl.when(a <= b)
            def _(ref=ref, tile=tile, a=a, b=b):
                work[b, pl.ds(pl.multiple_of(a * TILE, TILE), TILE), :] = ref[tile] * 2.0

            @pl.when(a > b)
            def _(ref=ref, tile=tile, a=a, b=b):
                work[a, pl.ds(pl.multiple_of(b * TILE, TILE), TILE), :] = ref[tile].T * 2.0

    row_of = lax.broadcasted_iota(jnp.int32, (8, TILE), 0)

    def one_block(j, carry):
        base = j * TILE

        def rows(i):
            return pl.ds(pl.multiple_of(base + 8 * i, 8), 8)

        for t in range(16):
            head = work[j, rows(t), :]
            columns = [over_lanes(head, 8 * t + m) for m in range(8)]
            roots, lefts, pairs = [], [], {}
            scale = jnp.zeros((8, TILE), F32)
            for m in range(8):
                root = inverse_root(over_rows(columns[m], m))
                column = columns[m] * root
                for q in range(m + 1, 8):
                    pairs[q, m] = over_rows(column, q)
                    columns[q] = columns[q] - column * pairs[q, m]
                roots.append(root)
                lefts.append(jnp.where(row_of > m, column, 0.0))
                scale = jnp.where(row_of == m, root, scale)
            for i in range(t + 1, 16):
                block = work[j, rows(i), :]
                got = []
                for m in range(8):
                    value = over_lanes(block, 8 * t + m)
                    for q in range(m):
                        value = value - got[q] * pairs[m, q]
                    got.append(value * roots[m])
                    left[i, m] = got[m]

            def one_tile(k, carry, t=t, lefts=lefts, roots=roots, scale=scale):
                head = work[k, rows(t), :]
                for m in range(8):
                    head = head - lefts[m] * (over_rows(head, m) * roots[m])
                head = head * scale
                work[k, rows(t), :] = head
                if t < 15:
                    lines = [over_rows(head, m) for m in range(8)]
                    for i in range(t + 1, 16):
                        block = work[k, rows(i), :]
                        for m in range(8):
                            block = block - left[i, m] * lines[m]
                        work[k, rows(i), :] = block
                return carry

            lax.fori_loop(j, 8, one_tile, 0)

        for done in range(7):

            @pl.when(j == done)
            def _(done=done):
                rows_done = slice(done * TILE, (done + 1) * TILE)
                for i in range(done + 1, 8):
                    turned_tile = work[i, rows_done, :].T
                    for k in range(i, 8):
                        into = slice(i * TILE, (i + 1) * TILE)
                        work[k, into, :] = work[k, into, :] - jnp.dot(
                            turned_tile,
                            work[k, rows_done, :],
                            precision=EXACT,
                            preferred_element_type=F32,
                        )

        return carry

    lax.fori_loop(0, 8, one_block, 0)
    count = out_ref.shape[0]
    row = row0 + lax.broadcasted_iota(jnp.int32, (count, TILE), 0)
    for k in range(8):
        col = k * TILE + lax.broadcasted_iota(jnp.int32, (count, TILE), 1)
        mine = work[k, pl.ds(pl.multiple_of(row0, count), count), :]
        out_ref[:, k * TILE : (k + 1) * TILE] = jnp.where(col >= row, mine, 0.0)


def factored(at, tiles, share):
    return pl.pallas_call(
        factor_kernel,
        in_specs=[pl.BlockSpec(memory_space=pltpu.SMEM)]
        + [pl.BlockSpec(memory_space=pltpu.VMEM)] * len(tiles),
        out_specs=pl.BlockSpec(memory_space=pltpu.VMEM),
        out_shape=jax.ShapeDtypeStruct((share, COLS), F32),
        scratch_shapes=[
            pltpu.VMEM((8, COLS, TILE), F32),
            pltpu.VMEM((16, 8, 8, TILE), F32),
        ],
        compiler_params=vmem(),
        name="factor",
    )(at, *tiles)


def from_ahead(array, axis, shift):
    size = lax.axis_size(axis)
    return lax.ppermute(array, axis, [((i + shift) % size, i) for i in range(size)])


def in_line(array, axis):
    size = lax.axis_size(axis)
    near = [array] + [from_ahead(array, axis, s) for s in range(1, size)]
    twice = jnp.stack(near + near)
    return lax.dynamic_slice_in_dim(twice, size - lax.axis_index(axis), size, 0)


def all_samples(samples):
    lines = samples
    for axis in ("c", "y", "x", "z"):
        lines = in_line(lines, axis)
    return lines.transpose(2, 3, 1, 0, 4).reshape(32, -1)


def shards(matrix, row_signs, samples):
    rows, cols = matrix.shape
    at_y, at_c = lax.axis_index("y"), lax.axis_index("c")
    at_z, at_x = lax.axis_index("z"), lax.axis_index("x")
    flat = turned(matrix, row_signs)
    blocks = lax.all_to_all(flat.reshape(32, 32, rows), PLANE, 0, 0, tiled=True)
    low, high = sampled_signs(at_z.reshape(1), all_samples(samples))
    ours = picked(blocks, low, high)
    arrived = lax.all_to_all(ours, ("z", "x"), 0, 0, tiled=True)
    own = arrived.reshape(8, TILE, 256).sum(axis=0)
    near, far = from_ahead(own, "y", 1), from_ahead(own, "y", 2)
    others = [from_ahead(a, "c", 1) for a in (own, near, far)]
    tiles = gram_tiles(own, near, far, *others).reshape(32, 24, TILE)
    share = lax.all_to_all(tiles, ("z", "x"), 0, 0, tiled=True).sum(axis=0)
    whole = jnp.broadcast_to(share[None], (32, 24, TILE))
    whole = lax.all_to_all(whole, ("z", "x"), 0, 0, tiled=True).reshape(6, TILE, TILE)
    lines = [whole, from_ahead(whole, "y", 1)]
    lines += [from_ahead(whole[:4], "y", 2), from_ahead(whole[:4], "y", 3)]
    lines += [from_ahead(a, "c", 1) for a in lines]
    out_rows = COLS // 32
    at = jnp.stack([at_y, at_c, (at_x * 8 + at_z) * out_rows]).astype(jnp.int32)
    return factored(at, lines, out_rows)


def solution(mesh):
    finer = Mesh(mesh.devices.reshape(4, 8, 4, 2), ALL)
    return jax.shard_map(
        shards,
        mesh=finer,
        in_specs=(P(ALL, None), P(ALL), P(ALL)),
        out_specs=P(("x", "z"), None),
        check_vma=False,
    )
```

```python
import functools

import jax
import jax.numpy as jnp
from jax import lax
from jax.experimental import pallas as pl
from jax.experimental.pallas import tpu as pltpu
from jax.sharding import Mesh
from jax.sharding import PartitionSpec as P

ALL = ("x", "z", "y", "c")
PLANE = ("y", "c", "x")
EXACT = lax.Precision.HIGHEST
F32 = jnp.float32
BF16 = jnp.bfloat16
COLS = 1024
BLOCKS = 256
TILE = 128
SHARE = 32
CHUNKS = (32,)
STEPS = 4


def vmem(limit=100):
    return pltpu.CompilerParams(vmem_limit_bytes=limit * 1024 * 1024 // 2)


def turn_kernel(sign_ref, in_ref, *out_refs):
    for t in range(in_ref.shape[0] // TILE):
        rows = slice(t * TILE, (t + 1) * TILE)
        lines = in_ref[rows, :].T * sign_ref[t : t + 1, :].astype(F32)
        for group in range(TILE // SHARE):
            first = group * SHARE
            for out_ref in out_refs:
                count = out_ref.shape[0] * SHARE // TILE
                into = slice(group * count, (group + 1) * count)
                out_ref[into, rows] = lines[first : first + count, :]
                first += count


def turned(matrix, row_signs):
    rows, cols = matrix.shape
    signs = row_signs.reshape(rows // TILE, TILE)
    groups = TILE // SHARE
    return pl.pallas_call(
        turn_kernel,
        grid=(cols // TILE,),
        in_specs=[
            pl.BlockSpec(signs.shape, lambda i: (0, 0)),
            pl.BlockSpec((rows, TILE), lambda i: (0, i)),
        ],
        out_specs=[pl.BlockSpec((groups * n, rows), lambda i: (i, 0)) for n in CHUNKS],
        out_shape=[jax.ShapeDtypeStruct((cols * n // SHARE, rows), F32) for n in CHUNKS],
        compiler_params=vmem(),
        name="turn",
    )(signs, matrix)


def odd_ones(bits, count):
    for shift in (8, 4, 2, 1):
        if shift < count:
            bits = bits ^ (bits >> shift)
    return bits & 1


def signs_kernel(z_ref, sample_ref, low_ref, high_ref):
    block = pl.program_id(0)
    within = sample_ref[pl.ds(block, 1), :] & 2047
    wl = lax.broadcasted_iota(jnp.int32, (256, 256), 0)
    low = odd_ones(wl & (within & 255), 8)
    low_ref[0] = (1 - 2 * low).astype(F32).astype(BF16)
    wh = lax.broadcasted_iota(jnp.int32, (8, 256), 0)
    lane = lax.broadcasted_iota(jnp.int32, (8, 256), 1)
    odd = odd_ones(wh & (within >> 8), 4) ^ odd_ones((lane >> 5) & z_ref[0], 4)
    high_ref[0] = (1 - 2 * odd).astype(F32) * (2.0**-7)


def sampled_signs(z_index, samples):
    return pl.pallas_call(
        signs_kernel,
        grid=(32,),
        in_specs=[
            pl.BlockSpec(memory_space=pltpu.SMEM),
            pl.BlockSpec((32, 256), lambda i: (0, 0)),
        ],
        out_specs=[
            pl.BlockSpec((1, 256, 256), lambda i: (i, 0, 0)),
            pl.BlockSpec((1, 8, 256), lambda i: (i, 0, 0)),
        ],
        out_shape=[
            jax.ShapeDtypeStruct((32, 256, 256), BF16),
            jax.ShapeDtypeStruct((32, 8, 256), F32),
        ],
        compiler_params=vmem(),
        name="signs",
    )(z_index, samples)


def butterflies(values):
    span = 1
    while span < len(values):
        new = list(values)
        for i in range(len(values)):
            if not i & span:
                new[i] = values[i] + values[i + span]
                new[i + span] = values[i] - values[i + span]
        values = new
        span *= 2
    return values


def pick_kernel(in_ref, low_ref, high_ref, out_ref, parts_ref):
    step = pl.program_id(0)
    count = in_ref.shape[1]

    @pl.when(step < STEPS)
    def _():
        for half in range(in_ref.shape[2] // 256):
            wh = step * (in_ref.shape[2] // 256) + half
            for row in range(0, count, 16):
                for lane in range(0, 256, TILE):
                    lanes = slice(lane, lane + TILE)
                    at = slice(half * 256 + lane, half * 256 + lane + TILE)
                    values = butterflies([in_ref[p, row : row + 16, at] for p in range(32)])
                    for p in range(32):
                        rest = values[p]
                        for part in range(3):
                            piece = rest.astype(BF16)
                            first = count * part + row
                            parts_ref[p, wh, first : first + 16, lanes] = piece
                            if part < 2:
                                rest = rest - piece.astype(F32)

    @pl.when(step >= STEPS)
    def _():
        for n in range(out_ref.shape[0]):
            p = (step - STEPS) * out_ref.shape[0] + n
            lines = parts_ref[p].reshape(24 * count, 256)
            got = jnp.dot(lines, low_ref[n], preferred_element_type=F32)
            total = jnp.zeros((count, 256), F32)
            for wh in range(8):
                some = got[3 * count * wh : 3 * count * (wh + 1)]
                some = some[0:count] + some[count : 2 * count] + some[2 * count :]
                total = total + some * high_ref[n, wh : wh + 1, :]
            out_ref[n] = total


def picked(blocks, low, high):
    count, rows = blocks.shape[1:]
    group = 32 // STEPS
    late = lambda i: (jnp.maximum(i - STEPS, 0), 0, 0)
    return pl.pallas_call(
        pick_kernel,
        grid=(2 * STEPS,),
        in_specs=[
            pl.BlockSpec(
                (32, count, rows // STEPS), lambda i: (0, 0, jnp.minimum(i, STEPS - 1))
            ),
            pl.BlockSpec((group, 256, 256), late),
            pl.BlockSpec((group, 8, 256), late),
        ],
        out_specs=pl.BlockSpec((group, count, 256), late),
        out_shape=jax.ShapeDtypeStruct((32, count, 256), F32),
        scratch_shapes=[pltpu.VMEM((32, 8, 3 * count, 256), BF16)],
        compiler_params=vmem(),
        name="pick",
    )(blocks, low, high)


def gram_kernel(own_ref, near_ref, far_ref, o_own_ref, o_near_ref, o_far_ref, out_ref):
    others = (own_ref, o_own_ref, near_ref, o_near_ref, far_ref, o_far_ref)
    for tile, other in enumerate(others):
        out_ref[tile] = lax.dot_general(
            own_ref[...],
            other[...],
            (((1,), (1,)), ((), ())),
            precision=EXACT,
            preferred_element_type=F32,
        )


def gram_tiles(*blocks):
    return pl.pallas_call(
        gram_kernel,
        out_shape=jax.ShapeDtypeStruct((6, TILE, TILE), F32),
        compiler_params=vmem(),
        name="gram",
    )(*blocks)


def over_lanes(block, lane):
    return jnp.broadcast_to(block[:, lane : lane + 1], (8, TILE))


def over_rows(block, row):
    return jnp.broadcast_to(block[row : row + 1, :], (8, TILE))


def inverse_root(d):
    root = lax.rsqrt(d)
    return root * (1.5 - 0.5 * (d * root) * root)


def factor_kernel(at_ref, *refs):
    tile_refs = refs[:8]
    out_ref, work, left, heads, scales = refs[8:]
    y, c, row0 = at_ref[0], at_ref[1], at_ref[2]
    for n, ref in enumerate(tile_refs):
        shift, other = n % 4, n // 4
        ys, cs = (y + shift) % 4, c ^ other
        a = 2 * ys + cs
        for tile in range(ref.shape[0]):
            dy, dc = tile // 2, tile % 2
            b = 2 * ((ys + dy) % 4) + (cs ^ dc)

            @pl.when(a <= b)
            def _(ref=ref, tile=tile, a=a, b=b):
                work[b, pl.ds(pl.multiple_of(a * TILE, TILE), TILE), :] = ref[tile] * 2.0

            @pl.when(a > b)
            def _(ref=ref, tile=tile, a=a, b=b):
                work[a, pl.ds(pl.multiple_of(b * TILE, TILE), TILE), :] = ref[tile].T * 2.0

    row_of = lax.broadcasted_iota(jnp.int32, (8, TILE), 0)

    def one_block(j, carry):
        base = j * TILE

        def rows(i):
            return pl.ds(pl.multiple_of(base + 8 * i, 8), 8)

        for above in range(1, 8):

            @pl.when(j == above)
            def _(above=above):
                deep = above * TILE
                mine = work[above, 0:deep, :].T
                for k in range(above, 8):
                    into = slice(deep, deep + TILE)
                    work[k, into, :] = work[k, into, :] - jnp.dot(
                        mine,
                        work[k, 0:deep, :],
                        precision=EXACT,
                        preferred_element_type=F32,
                    )

        tile = [work[j, rows(i), :] for i in range(16)]
        columns = [over_lanes(tile[0], m) for m in range(8)]
        for t in range(16):
            head = tile[t]
            nexts = []
            if t < 15:
                nexts = [over_lanes(tile[t + 1], 8 * (t + 1) + q) for q in range(8)]
            inverses, pairs = [], {}
            scale = jnp.zeros((8, TILE), F32)
            for m in range(8):
                pivot = over_rows(columns[m], m)
                inverse = 1.0 / pivot
                for q in range(m + 1, 8):
                    entry = over_rows(columns[m], q)
                    columns[q] = columns[q] - (columns[m] * entry) * inverse
                    pairs[q, m] = entry * inverse
                masked = jnp.where(row_of > m, columns[m] * inverse, 0.0)
                heads[t, m] = masked
                head = head - masked * over_rows(head, m)
                inverses.append(inverse)
                scale = jnp.where(row_of == m, inverse_root(pivot), scale)
            scales[t] = scale
            work[j, rows(t), :] = head * scale
            lines = [over_rows(head, m) for m in range(8)]
            for i in range(t + 1, 16):
                got, scaled = [], []
                for m in range(8):
                    value = over_lanes(tile[i], 8 * t + m)
                    for q in range(m):
                        value = value - got[q] * pairs[m, q]
                    got.append(value)
                    scaled.append(value * inverses[m])
                    left[t, i, m] = scaled[m]
                for m in range(8):
                    tile[i] = tile[i] - scaled[m] * lines[m]
                if i == t + 1:
                    for q in range(8):
                        for m in range(8):
                            nexts[q] = nexts[q] - scaled[m] * over_rows(got[m], q)
            columns = nexts

        def one_tile(k, carry):
            lower = [work[k, rows(i), :] for i in range(16)]
            for t in range(16):
                head = lower[t]
                for m in range(8):
                    head = head - heads[t, m] * over_rows(head, m)
                work[k, rows(t), :] = head * scales[t]
                if t < 15:
                    lines = [over_rows(head, m) for m in range(8)]
                    for i in range(t + 1, 16):
                        for m in range(8):
                            lower[i] = lower[i] - left[t, i, m] * lines[m]
            return carry

        lax.fori_loop(j + 1, 8, one_tile, 0)
        return carry

    lax.fori_loop(0, 8, one_block, 0)
    count = out_ref.shape[0]
    row = row0 + lax.broadcasted_iota(jnp.int32, (count, TILE), 0)
    for k in range(8):
        col = k * TILE + lax.broadcasted_iota(jnp.int32, (count, TILE), 1)
        mine = work[k, pl.ds(pl.multiple_of(row0, count), count), :]
        out_ref[:, k * TILE : (k + 1) * TILE] = jnp.where(col >= row, mine, 0.0)


def factored(at, tiles, share):
    return pl.pallas_call(
        factor_kernel,
        in_specs=[pl.BlockSpec(memory_space=pltpu.SMEM)]
        + [pl.BlockSpec(memory_space=pltpu.VMEM)] * len(tiles),
        out_specs=pl.BlockSpec(memory_space=pltpu.VMEM),
        out_shape=jax.ShapeDtypeStruct((share, COLS), F32),
        scratch_shapes=[
            pltpu.VMEM((8, COLS, TILE), F32),
            pltpu.VMEM((16, 16, 8, 8, TILE), F32),
            pltpu.VMEM((16, 8, 8, TILE), F32),
            pltpu.VMEM((16, 8, TILE), F32),
        ],
        compiler_params=vmem(),
        name="factor",
    )(at, *tiles)


def from_ahead(array, axis, shift):
    size = lax.axis_size(axis)
    return lax.ppermute(array, axis, [((i + shift) % size, i) for i in range(size)])


def in_line(array, axis):
    size = lax.axis_size(axis)
    near = [array] + [from_ahead(array, axis, s) for s in range(1, size)]
    twice = jnp.stack(near + near)
    return lax.dynamic_slice_in_dim(twice, size - lax.axis_index(axis), size, 0)


def all_samples(samples):
    lines = jnp.broadcast_to(samples[None, None], (32, 1, samples.shape[0]))
    lines = lax.all_to_all(lines, PLANE, 0, 0, tiled=True)
    return in_line(lines, "z").transpose(1, 0, 2, 3).reshape(32, -1)


def shards(matrix, row_signs, samples):
    rows, cols = matrix.shape
    at_y, at_c = lax.axis_index("y"), lax.axis_index("c")
    at_z, at_x = lax.axis_index("z"), lax.axis_index("x")
    low, high = sampled_signs(at_z.reshape(1), all_samples(samples))
    flats = turned(matrix, row_signs)
    own = []
    for n, (flat, count) in enumerate(zip(flats, CHUNKS)):
        if n == 1:
            flat, low, high = lax.optimization_barrier((flat, low, high))
        blocks = lax.all_to_all(flat.reshape(32, count, rows), PLANE, 0, 0, tiled=True)
        ours = picked(blocks, low, high)
        arrived = lax.all_to_all(ours, ("z", "x"), 0, 0, tiled=True)
        own.append(arrived.reshape(8, 4, count, 256).sum(axis=0))
    own = jnp.concatenate(own, axis=1).reshape(TILE, 256)
    near, far = from_ahead(own, "y", 1), from_ahead(own, "y", 2)
    others = [from_ahead(a, "c", 1) for a in (own, near, far)]
    tiles = gram_tiles(own, near, far, *others).reshape(32, 24, TILE)
    share = lax.all_to_all(tiles, ("z", "x"), 0, 0, tiled=True).sum(axis=0)
    whole = jnp.broadcast_to(share[None], (32, 24, TILE))
    whole = lax.all_to_all(whole, ("z", "x"), 0, 0, tiled=True).reshape(6, TILE, TILE)
    lines = [whole, from_ahead(whole, "y", 1)]
    lines += [from_ahead(whole[:4], "y", 2), from_ahead(whole[:4], "y", 3)]
    lines += [from_ahead(a, "c", 1) for a in lines]
    out_rows = COLS // 32
    at = jnp.stack([at_y, at_c, (at_x * 8 + at_z) * out_rows]).astype(jnp.int32)
    return factored(at, lines, out_rows)


def solution(mesh):
    finer = Mesh(mesh.devices.reshape(4, 8, 4, 2), ALL)
    return jax.shard_map(
        shards,
        mesh=finer,
        in_specs=(P(ALL, None), P(ALL), P(ALL)),
        out_specs=P(("x", "z"), None),
        check_vma=False,
    )
```

```python
import functools

import jax
import jax.numpy as jnp
from jax import lax
from jax.experimental import pallas as pl
from jax.experimental.pallas import tpu as pltpu
from jax.sharding import Mesh
from jax.sharding import PartitionSpec as P

ALL = ("x", "z", "y", "c")
PLANE = ("y", "c", "x")
EXACT = lax.Precision.HIGHEST
F32 = jnp.float32
BF16 = jnp.bfloat16
COLS = 1024
TILE = 128
NEAR = 24
FAR = 32
WIDTH = 2
STEPS = 4


def vmem(limit=100):
    return pltpu.CompilerParams(vmem_limit_bytes=limit * 1024 * 1024 // 2)


def turn_kernel(z_ref, sign_ref, in_ref, near_ref, far_ref):
    del z_ref
    for t in range(in_ref.shape[0] // TILE):
        rows = slice(t * TILE, (t + 1) * TILE)
        lines = in_ref[rows, :].T * sign_ref[t : t + 1, :].astype(F32)
        near_ref[:, rows] = lines[: 4 * NEAR, :]
        far_ref[0, :, rows] = lines[4 * NEAR :, :]


def turned(z_index, matrix, row_signs):
    rows, cols = matrix.shape
    signs = row_signs.reshape(rows // TILE, TILE)
    return pl.pallas_call(
        turn_kernel,
        grid_spec=pltpu.PrefetchScalarGridSpec(
            num_scalar_prefetch=1,
            grid=(cols // TILE,),
            in_specs=[
                pl.BlockSpec(signs.shape, lambda i, z: (0, 0)),
                pl.BlockSpec((rows, TILE), lambda i, z: (0, i)),
            ],
            out_specs=[
                pl.BlockSpec((4 * NEAR, rows), lambda i, z: (i, 0)),
                pl.BlockSpec((1, FAR, rows), lambda i, z: (i ^ z[0], 0, 0)),
            ],
        ),
        out_shape=[
            jax.ShapeDtypeStruct((32 * NEAR, rows), F32),
            jax.ShapeDtypeStruct((8, FAR, rows), F32),
        ],
        compiler_params=vmem(),
        name="turn",
    )(z_index, signs, matrix)


def odd_ones(bits):
    for shift in (4, 2, 1):
        bits = bits ^ (bits >> shift)
    return bits & 1


def signs_kernel(at_ref, sample_ref, low_ref, high_ref):
    block = pl.program_id(0)
    count = low_ref.shape[2]
    within = sample_ref[pl.ds(block, 1), :] & 2047
    for lane in range(0, count, 256):
        lanes = slice(lane, lane + 256)
        wl = lax.broadcasted_iota(jnp.int32, (256, 256), 0)
        low = odd_ones(wl & (within[:, lanes] & 255))
        low_ref[0, :, lanes] = (1 - 2 * low).astype(F32).astype(BF16)
    wh = lax.broadcasted_iota(jnp.int32, (8, count), 0)
    lane = lax.broadcasted_iota(jnp.int32, (8, count), 1)
    odd = odd_ones(wh & (within >> 8)) ^ odd_ones((lane >> 5) & at_ref[0])
    odd = odd ^ odd_ones(block & at_ref[1])
    high_ref[0] = (1 - 2 * odd).astype(F32) * (2.0**-7)


def sampled_signs(at, samples):
    blocks, count = samples.shape
    return pl.pallas_call(
        signs_kernel,
        grid=(blocks,),
        in_specs=[
            pl.BlockSpec(memory_space=pltpu.SMEM),
            pl.BlockSpec((blocks, count), lambda i: (0, 0)),
        ],
        out_specs=[
            pl.BlockSpec((1, 256, count), lambda i: (i, 0, 0)),
            pl.BlockSpec((1, 8, count), lambda i: (i, 0, 0)),
        ],
        out_shape=[
            jax.ShapeDtypeStruct((blocks, 256, count), BF16),
            jax.ShapeDtypeStruct((blocks, 8, count), F32),
        ],
        compiler_params=vmem(),
        name="signs",
    )(at, samples)


def butterflies(values):
    span = 1
    while span < len(values):
        new = list(values)
        for i in range(len(values)):
            if not i & span:
                new[i] = values[i] + values[i + span]
                new[i + span] = values[i] - values[i + span]
        values = new
        span *= 2
    return values


def mix_blocks(step, read, count, cols, parts_ref):
    pieces = [(wh, col) for wh in range(2) for col in range(0, cols, 8)]
    for n in range(0, len(pieces), 2):
        for lane in range(0, 256, TILE):
            both = []
            for wh, col in pieces[n : n + 2]:
                first = 256 * wh + lane
                lanes = slice(first, first + TILE)
                both.append([read(p, slice(col, col + 8), lanes) for p in range(count)])
            values = [jnp.concatenate(pair, axis=0) for pair in zip(*both)]
            for p, rest in enumerate(butterflies(values)):
                for part in range(3):
                    piece = rest.astype(BF16)
                    parts_ref[p, part, step, 8 * n : 8 * n + 16, lane : lane + TILE] = piece
                    if part < 2:
                        rest = rest - piece.astype(F32)


def pick_rows(lines, low, high, cols):
    got = jnp.dot(lines, low, preferred_element_type=F32)
    size = 8 * cols
    got = got[:size] + got[size : 2 * size] + got[2 * size :]
    total = got[:cols] * high[0:1]
    for wh in range(1, 8):
        total = total + got[cols * wh : cols * (wh + 1)] * high[wh : wh + 1]
    return total


def near_kernel(in_ref, low_ref, high_ref, out_ref, parts_ref, rows_ref):
    step = pl.program_id(0)

    @pl.when(step < STEPS)
    def _():
        read = lambda p, cols, lanes: in_ref[p, cols, lanes]
        mix_blocks(step, read, 32, NEAR, parts_ref)

    @pl.when(step >= STEPS)
    def _():
        def one(n, carry):
            lines = parts_ref[(step - STEPS) * 8 + n].reshape(24 * NEAR, 256)
            rows_ref[n] = pick_rows(lines, low_ref[n], high_ref[n], NEAR)
            return carry

        lax.fori_loop(0, 8, one, 0, unroll=2)
        group = lax.broadcasted_iota(jnp.int32, (NEAR, TILE), 1) >> 5
        for z in range(8):
            lanes = slice(TILE * (z // 4), TILE * (z // 4) + TILE)
            for half in range(2):
                total = jnp.zeros((NEAR, TILE), F32)
                for n in range(4):
                    block = rows_ref[4 * half + n, :, lanes]
                    block = pltpu.roll(block, (32 * n - 32 * (z % 4)) % TILE, 1)
                    total = jnp.where(group == n, block, total)
                out_ref[0, z, :, TILE * half : TILE * half + TILE] = total


def late(i):
    return jnp.maximum(i - STEPS, 0)


def early(i):
    return jnp.minimum(i, STEPS - 1)


def near_picked(blocks, low, high):
    wide = blocks.shape[2] // STEPS
    return pl.pallas_call(
        near_kernel,
        grid=(2 * STEPS,),
        in_specs=[
            pl.BlockSpec((32, NEAR, wide), lambda i: (0, 0, early(i))),
            pl.BlockSpec((8, 256, 256), lambda i: (late(i), 0, 0)),
            pl.BlockSpec((8, 8, 256), lambda i: (late(i), 0, 0)),
        ],
        out_specs=pl.BlockSpec((1, 8, NEAR, 256), lambda i: (late(i), 0, 0, 0)),
        out_shape=jax.ShapeDtypeStruct((4, 8, NEAR, 256), F32),
        scratch_shapes=[
            pltpu.VMEM((32, 3, STEPS, 2 * NEAR, 256), BF16),
            pltpu.VMEM((8, NEAR, 256), F32),
        ],
        compiler_params=vmem(),
        name="near",
    )(blocks, low, high)


def far_kernel(*refs):
    in_refs = refs[:8]
    low_ref, high_ref, out_ref, parts_ref = refs[8:]
    step = pl.program_id(0)

    @pl.when(step < STEPS)
    def _():
        read = lambda p, cols, lanes: in_refs[p][cols, lanes]
        mix_blocks(step, read, 8, FAR, parts_ref)

    @pl.when(step >= STEPS)
    def _():
        def one(n, carry):
            lines = parts_ref[(step - STEPS) * 2 + n].reshape(24 * FAR, 256)
            for q in range(4):
                lanes = slice(256 * q, 256 * q + 256)
                out_ref[q, n] = pick_rows(lines, low_ref[n, :, lanes], high_ref[n, :, lanes], FAR)
            return carry

        lax.fori_loop(0, 2, one, 0)


def far_picked(pieces, low, high):
    wide = pieces[0].shape[1] // STEPS
    return pl.pallas_call(
        far_kernel,
        grid=(2 * STEPS,),
        in_specs=[pl.BlockSpec((FAR, wide), lambda i: (0, early(i)))] * 8
        + [
            pl.BlockSpec((2, 256, 1024), lambda i: (late(i), 0, 0)),
            pl.BlockSpec((2, 8, 1024), lambda i: (late(i), 0, 0)),
        ],
        out_specs=pl.BlockSpec((4, 2, FAR, 256), lambda i: (0, late(i), 0, 0)),
        out_shape=jax.ShapeDtypeStruct((4, 8, FAR, 256), F32),
        scratch_shapes=[pltpu.VMEM((8, 3, STEPS, 2 * FAR, 256), BF16)],
        compiler_params=vmem(),
        name="far",
    )(*pieces, low, high)


def gram_kernel(own_ref, near_ref, far_ref, o_own_ref, o_near_ref, o_far_ref, out_ref):
    others = (own_ref, o_own_ref, near_ref, o_near_ref, far_ref, o_far_ref)
    for tile, other in enumerate(others):
        out_ref[tile] = lax.dot_general(
            own_ref[...],
            other[...],
            (((1,), (1,)), ((), ())),
            precision=EXACT,
            preferred_element_type=F32,
        )


def gram_tiles(*blocks):
    return pl.pallas_call(
        gram_kernel,
        out_shape=jax.ShapeDtypeStruct((6, TILE, TILE), F32),
        compiler_params=vmem(),
        name="gram",
    )(*blocks)


def over_lanes(block, lane):
    return jnp.broadcast_to(block[:, lane : lane + 1], (8, TILE))


def over_rows(block, row):
    return jnp.broadcast_to(block[row : row + 1, :], (8, TILE))


def inverse_root(d):
    root = lax.rsqrt(d)
    return root


def factor_kernel(at_ref, *refs):
    tile_refs = refs[:8]
    out_ref, work, left, heads, scales = refs[8:]
    y, c, row0 = at_ref[0], at_ref[1], at_ref[2]
    for n, ref in enumerate(tile_refs):
        shift, other = n % 4, n // 4
        ys, cs = (y + shift) % 4, c ^ other
        a = 2 * ys + cs
        for tile in range(ref.shape[0]):
            dy, dc = tile // 2, tile % 2
            b = 2 * ((ys + dy) % 4) + (cs ^ dc)

            @pl.when(a <= b)
            def _(ref=ref, tile=tile, a=a, b=b):
                work[b, pl.ds(pl.multiple_of(a * TILE, TILE), TILE), :] = ref[tile] * 2.0

            @pl.when(a > b)
            def _(ref=ref, tile=tile, a=a, b=b):
                work[a, pl.ds(pl.multiple_of(b * TILE, TILE), TILE), :] = ref[tile].T * 2.0

    row_of = lax.broadcasted_iota(jnp.int32, (8, TILE), 0)

    def one_block(j, carry):
        base = j * TILE

        def rows(i):
            return pl.ds(pl.multiple_of(base + 8 * i, 8), 8)

        for above in range(1, 8):

            @pl.when(j == above)
            def _(above=above):
                deep = above * TILE
                mine = work[above, 0:deep, :].T
                for k in range(above, 8):
                    into = slice(deep, deep + TILE)
                    work[k, into, :] = work[k, into, :] - jnp.dot(
                        mine,
                        work[k, 0:deep, :],
                        precision=EXACT,
                        preferred_element_type=F32,
                    )

        tile = [work[j, rows(i), :] for i in range(16)]
        columns = [over_lanes(tile[0], m) for m in range(8)]
        for t in range(16):
            head = tile[t]
            nexts = []
            if t < 15:
                nexts = [over_lanes(tile[t + 1], 8 * (t + 1) + q) for q in range(8)]
            roots, pairs = [], {}
            scale = jnp.zeros((8, TILE), F32)
            for m in range(8):
                root = inverse_root(over_rows(columns[m], m))
                column = columns[m] * root
                for q in range(m + 1, 8):
                    pairs[q, m] = over_rows(columns[m], q) * root
                    columns[q] = columns[q] - column * pairs[q, m]
                masked = jnp.where(row_of > m, column * root, 0.0)
                heads[t, m] = masked
                head = head - masked * over_rows(head, m)
                roots.append(root)
                scale = jnp.where(row_of == m, root, scale)
            scales[t] = scale
            head = head * scale
            work[j, rows(t), :] = head
            lines = [over_rows(head, m) for m in range(8)]
            if t + 16 < 15:
                turned_head = head.T
            for i in range(t + 1, 16):
                got = []
                for m in range(8):
                    if i <= t + 16:
                        value = over_lanes(tile[i], 8 * t + m)
                        for q in range(m):
                            value = value - got[q] * pairs[m, q]
                        value = value * roots[m]
                    else:
                        value = jnp.broadcast_to(turned_head[8 * i : 8 * i + 8, m : m + 1], (8, TILE))
                    got.append(value)
                    left[t, i, m] = value
                for m in range(8):
                    tile[i] = tile[i] - got[m] * lines[m]
                if i == t + 1:
                    for q in range(8):
                        for m in range(8):
                            nexts[q] = nexts[q] - got[m] * over_rows(got[m], q)
            columns = nexts

        def some_tiles(n, carry):
            tiles = [j + 1 + n * WIDTH + w for w in range(WIDTH)]
            lower = [[work[k, rows(i), :] for i in range(16)] for k in tiles]
            for t in range(16):
                lines = []
                heads_now = [lower[w][t] for w in range(WIDTH)]
                for m in range(8):
                    column = heads[t, m]
                    for w in range(WIDTH):
                        heads_now[w] = heads_now[w] - column * over_rows(heads_now[w], m)
                for w in range(WIDTH):
                    done = heads_now[w] * scales[t]
                    work[tiles[w], rows(t), :] = done
                    lines.append([over_rows(done, m) for m in range(8)])
                for i in range(t + 1, 16):
                    for m in range(8):
                        column = left[t, i, m]
                        for w in range(WIDTH):
                            lower[w][i] = lower[w][i] - column * lines[w][m]
            return carry

        lax.fori_loop(0, (7 - j + WIDTH - 1) // WIDTH, some_tiles, 0)
        return carry

    lax.fori_loop(0, 8, one_block, 0)
    count = out_ref.shape[0]
    row = row0 + lax.broadcasted_iota(jnp.int32, (count, TILE), 0)
    for k in range(8):
        col = k * TILE + lax.broadcasted_iota(jnp.int32, (count, TILE), 1)
        mine = work[k, pl.ds(pl.multiple_of(row0, count), count), :]
        out_ref[:, k * TILE : (k + 1) * TILE] = jnp.where(col >= row, mine, 0.0)


def factored(at, tiles, share):
    return pl.pallas_call(
        factor_kernel,
        in_specs=[pl.BlockSpec(memory_space=pltpu.SMEM)]
        + [pl.BlockSpec(memory_space=pltpu.VMEM)] * len(tiles),
        out_specs=pl.BlockSpec(memory_space=pltpu.VMEM),
        out_shape=jax.ShapeDtypeStruct((share, COLS), F32),
        scratch_shapes=[
            pltpu.VMEM((7 + WIDTH, COLS, TILE), F32),
            pltpu.VMEM((16, 16, 8, 8, TILE), F32),
            pltpu.VMEM((16, 8, 8, TILE), F32),
            pltpu.VMEM((16, 8, TILE), F32),
        ],
        compiler_params=vmem(),
        name="factor",
    )(at, *tiles)


def from_ahead(array, axis, shift):
    size = lax.axis_size(axis)
    return lax.ppermute(array, axis, [((i + shift) % size, i) for i in range(size)])


def in_line(array, axis):
    lines = array[None]
    for bit in (1, 2, 4):
        other = lax.ppermute(lines, axis, [(i, i ^ bit) for i in range(8)])
        low = lax.axis_index(axis) & bit == 0
        lines = jnp.concatenate([jnp.where(low, lines, other), jnp.where(low, other, lines)])
    return lines


def all_samples(samples):
    lines = jnp.broadcast_to(samples[None, None], (32, 1, samples.shape[0]))
    lines = lax.all_to_all(lines, PLANE, 0, 0, tiled=True)
    return in_line(lines, "z").reshape(8, 32, -1)


def shards(matrix, row_signs, samples):
    rows, cols = matrix.shape
    at_y, at_c = lax.axis_index("y"), lax.axis_index("c")
    at_z, at_x = lax.axis_index("z"), lax.axis_index("x")
    drawn = all_samples(samples)
    first, second = turned(at_z.reshape(1), matrix, row_signs)
    blocks = lax.all_to_all(first.reshape(32, NEAR, rows), PLANE, 0, 0, tiled=True)
    drawn, second = lax.optimization_barrier((drawn, second))
    pieces = [second[0]]
    for s in range(1, 8):
        pieces.append(lax.ppermute(second[s], "z", [(i, i ^ s) for i in range(8)]))
    at = jnp.stack([at_z, jnp.zeros_like(at_z)]).astype(jnp.int32)
    near_signs = sampled_signs(at, drawn.transpose(1, 0, 2).reshape(32, -1))
    at = jnp.stack([lax.axis_index(PLANE), at_z]).astype(jnp.int32)
    far_signs = sampled_signs(at, drawn.reshape(8, -1))
    far_signs, near_signs = lax.optimization_barrier((far_signs, near_signs))
    ours = far_picked(pieces, *far_signs).reshape(32, FAR, 256)
    ours = lax.all_to_all(ours, ("x", "y", "c"), 0, 0, tiled=True).sum(axis=0)
    swap = [(8 * i + j, 8 * j + i) for i in range(8) for j in range(8)]
    others = lax.ppermute(ours, ("z", "y", "c"), swap)
    ours = near_picked(blocks, *near_signs).reshape(32, NEAR, 256)
    arrived = lax.all_to_all(ours, ("x", "z"), 0, 0, tiled=True)
    own = arrived.reshape(4, 8, NEAR, 256).sum(axis=1).reshape(4 * NEAR, 256)
    own = jnp.concatenate([own, others], axis=0)
    near, far = from_ahead(own, "y", 1), from_ahead(own, "y", 2)
    others = [from_ahead(a, "c", 1) for a in (own, near, far)]
    tiles = gram_tiles(own, near, far, *others).reshape(32, 24, TILE)
    share = lax.all_to_all(tiles, ("z", "x"), 0, 0, tiled=True).sum(axis=0)
    whole = jnp.broadcast_to(share[None], (32, 24, TILE))
    whole = lax.all_to_all(whole, ("z", "x"), 0, 0, tiled=True).reshape(6, TILE, TILE)
    lines = [whole, from_ahead(whole, "y", 1)]
    lines += [from_ahead(whole[:4], "y", 2), from_ahead(whole[:4], "y", 3)]
    lines += [from_ahead(a, "c", 1) for a in lines]
    out_rows = COLS // 32
    at = jnp.stack([at_y, at_c, (at_x * 8 + at_z) * out_rows]).astype(jnp.int32)
    return factored(at, lines, out_rows)


def solution(mesh):
    finer = Mesh(mesh.devices.reshape(4, 8, 4, 2), ALL)
    return jax.shard_map(
        shards,
        mesh=finer,
        in_specs=(P(ALL, None), P(ALL), P(ALL)),
        out_specs=P(("x", "z"), None),
        check_vma=False,
    )
```

```python
import functools

import jax
import jax.numpy as jnp
from jax import lax
from jax.experimental import pallas as pl
from jax.experimental.pallas import tpu as pltpu
from jax.sharding import Mesh
from jax.sharding import PartitionSpec as P

ALL = ("x", "z", "y", "c")
PLANE = ("y", "c", "x")
EXACT = lax.Precision.HIGHEST
F32 = jnp.float32
BF16 = jnp.bfloat16
COLS = 1024
TILE = 128
NEAR = 24
FAR = 32
STEPS = 4


def vmem(limit=100):
    return pltpu.CompilerParams(vmem_limit_bytes=limit * 1024 * 1024 // 2)


def turn_kernel(z_ref, sign_ref, in_ref, near_ref, far_ref):
    del z_ref
    for t in range(in_ref.shape[0] // TILE):
        rows = slice(t * TILE, (t + 1) * TILE)
        lines = in_ref[rows, :].T * sign_ref[t : t + 1, :].astype(F32)
        near_ref[:, rows] = lines[: 4 * NEAR, :]
        far_ref[0, :, rows] = lines[4 * NEAR :, :]


def turned(z_index, matrix, row_signs):
    rows, cols = matrix.shape
    signs = row_signs.reshape(rows // TILE, TILE)
    return pl.pallas_call(
        turn_kernel,
        grid_spec=pltpu.PrefetchScalarGridSpec(
            num_scalar_prefetch=1,
            grid=(cols // TILE,),
            in_specs=[
                pl.BlockSpec(signs.shape, lambda i, z: (0, 0)),
                pl.BlockSpec((rows, TILE), lambda i, z: (0, i)),
            ],
            out_specs=[
                pl.BlockSpec((4 * NEAR, rows), lambda i, z: (i, 0)),
                pl.BlockSpec((1, FAR, rows), lambda i, z: (i ^ z[0], 0, 0)),
            ],
        ),
        out_shape=[
            jax.ShapeDtypeStruct((32 * NEAR, rows), F32),
            jax.ShapeDtypeStruct((8, FAR, rows), F32),
        ],
        compiler_params=vmem(),
        name="turn",
    )(z_index, signs, matrix)


def odd_ones(bits):
    for shift in (4, 2, 1):
        bits = bits ^ (bits >> shift)
    return bits & 1


def signs_kernel(at_ref, sample_ref, low_ref, high_ref):
    block = pl.program_id(0)
    count = low_ref.shape[2]
    within = sample_ref[pl.ds(block, 1), :] & 2047
    for lane in range(0, count, 256):
        lanes = slice(lane, lane + 256)
        wl = lax.broadcasted_iota(jnp.int32, (256, 256), 0)
        low = odd_ones(wl & (within[:, lanes] & 255))
        low_ref[0, :, lanes] = (1 - 2 * low).astype(F32).astype(BF16)
    wh = lax.broadcasted_iota(jnp.int32, (8, count), 0)
    lane = lax.broadcasted_iota(jnp.int32, (8, count), 1)
    odd = odd_ones(wh & (within >> 8)) ^ odd_ones((lane >> 5) & at_ref[0])
    odd = odd ^ odd_ones(block & at_ref[1])
    high_ref[0] = (1 - 2 * odd).astype(F32) * (2.0**-7)


def sampled_signs(at, samples):
    blocks, count = samples.shape
    return pl.pallas_call(
        signs_kernel,
        grid=(blocks,),
        in_specs=[
            pl.BlockSpec(memory_space=pltpu.SMEM),
            pl.BlockSpec((blocks, count), lambda i: (0, 0)),
        ],
        out_specs=[
            pl.BlockSpec((1, 256, count), lambda i: (i, 0, 0)),
            pl.BlockSpec((1, 8, count), lambda i: (i, 0, 0)),
        ],
        out_shape=[
            jax.ShapeDtypeStruct((blocks, 256, count), BF16),
            jax.ShapeDtypeStruct((blocks, 8, count), F32),
        ],
        compiler_params=vmem(),
        name="signs",
    )(at, samples)


def butterflies(values):
    span = 1
    while span < len(values):
        new = list(values)
        for i in range(len(values)):
            if not i & span:
                new[i] = values[i] + values[i + span]
                new[i + span] = values[i] - values[i + span]
        values = new
        span *= 2
    return values


def mix_blocks(step, read, count, cols, parts_ref):
    pieces = [(wh, col) for wh in range(2) for col in range(0, cols, 8)]
    for n in range(0, len(pieces), 2):
        for lane in range(0, 256, TILE):
            both = []
            for wh, col in pieces[n : n + 2]:
                first = 256 * wh + lane
                lanes = slice(first, first + TILE)
                both.append([read(p, slice(col, col + 8), lanes) for p in range(count)])
            values = [jnp.concatenate(pair, axis=0) for pair in zip(*both)]
            for p, rest in enumerate(butterflies(values)):
                for part in range(3):
                    piece = rest.astype(BF16)
                    parts_ref[p, part, step, 8 * n : 8 * n + 16, lane : lane + TILE] = piece
                    if part < 2:
                        rest = rest - piece.astype(F32)


def pick_rows(lines, low, high, cols):
    got = jnp.dot(lines, low, preferred_element_type=F32)
    size = 8 * cols
    got = got[:size] + got[size : 2 * size] + got[2 * size :]
    total = got[:cols] * high[0:1]
    for wh in range(1, 8):
        total = total + got[cols * wh : cols * (wh + 1)] * high[wh : wh + 1]
    return total


def near_kernel(in_ref, low_ref, high_ref, out_ref, parts_ref, rows_ref):
    step = pl.program_id(0)

    @pl.when(step < STEPS)
    def _():
        read = lambda p, cols, lanes: in_ref[p, cols, lanes]
        mix_blocks(step, read, 32, NEAR, parts_ref)

    @pl.when(step >= STEPS)
    def _():
        def one(n, carry):
            lines = parts_ref[(step - STEPS) * 8 + n].reshape(24 * NEAR, 256)
            rows_ref[n] = pick_rows(lines, low_ref[n], high_ref[n], NEAR)
            return carry

        lax.fori_loop(0, 8, one, 0, unroll=2)
        group = lax.broadcasted_iota(jnp.int32, (NEAR, TILE), 1) >> 5
        for z in range(8):
            lanes = slice(TILE * (z // 4), TILE * (z // 4) + TILE)
            for half in range(2):
                total = jnp.zeros((NEAR, TILE), F32)
                for n in range(4):
                    block = rows_ref[4 * half + n, :, lanes]
                    block = pltpu.roll(block, (32 * n - 32 * (z % 4)) % TILE, 1)
                    total = jnp.where(group == n, block, total)
                out_ref[0, z, :, TILE * half : TILE * half + TILE] = total


def late(i):
    return jnp.maximum(i - STEPS, 0)


def early(i):
    return jnp.minimum(i, STEPS - 1)


def near_picked(blocks, low, high):
    wide = blocks.shape[2] // STEPS
    return pl.pallas_call(
        near_kernel,
        grid=(2 * STEPS,),
        in_specs=[
            pl.BlockSpec((32, NEAR, wide), lambda i: (0, 0, early(i))),
            pl.BlockSpec((8, 256, 256), lambda i: (late(i), 0, 0)),
            pl.BlockSpec((8, 8, 256), lambda i: (late(i), 0, 0)),
        ],
        out_specs=pl.BlockSpec((1, 8, NEAR, 256), lambda i: (late(i), 0, 0, 0)),
        out_shape=jax.ShapeDtypeStruct((4, 8, NEAR, 256), F32),
        scratch_shapes=[
            pltpu.VMEM((32, 3, STEPS, 2 * NEAR, 256), BF16),
            pltpu.VMEM((8, NEAR, 256), F32),
        ],
        compiler_params=vmem(),
        name="near",
    )(blocks, low, high)


def far_kernel(at_ref, *refs):
    in_refs = refs[:8]
    low_ref, high_ref, out_ref, parts_ref = refs[8:]
    step = pl.program_id(0)

    @pl.when(step < STEPS)
    def _():
        read = lambda p, cols, lanes: in_refs[p][cols, lanes]
        mix_blocks(step, read, 8, FAR, parts_ref)

    @pl.when(step >= STEPS)
    def _():
        def one(n, carry):
            lines = parts_ref[(step - STEPS) * 2 + n].reshape(24 * FAR, 256)
            for q in range(4):
                lanes = slice(256 * q, 256 * q + 256)
                got = pick_rows(lines, low_ref[n, :, lanes], high_ref[n, :, lanes], FAR)
                out_ref[q ^ at_ref[0], n ^ at_ref[2]] = got
            return carry

        lax.fori_loop(0, 2, one, 0)


def far_picked(at, pieces, low, high):
    wide = pieces[0].shape[1] // STEPS
    return pl.pallas_call(
        far_kernel,
        grid_spec=pltpu.PrefetchScalarGridSpec(
            num_scalar_prefetch=1,
            grid=(2 * STEPS,),
            in_specs=[pl.BlockSpec((FAR, wide), lambda i, at: (0, early(i)))] * 8
            + [
                pl.BlockSpec((2, 256, 1024), lambda i, at: (late(i), 0, 0)),
                pl.BlockSpec((2, 8, 1024), lambda i, at: (late(i), 0, 0)),
            ],
            out_specs=pl.BlockSpec(
                (4, 2, FAR, 256), lambda i, at: (0, late(i) ^ at[1], 0, 0)
            ),
            scratch_shapes=[pltpu.VMEM((8, 3, STEPS, 2 * FAR, 256), BF16)],
        ),
        out_shape=jax.ShapeDtypeStruct((4, 8, FAR, 256), F32),
        compiler_params=vmem(),
        name="far",
    )(at, *pieces, low, high)


def sum_of_pieces(pieces, axis):
    total = pieces[0]
    size = len(pieces)
    for r in range(1, size):
        total = total + lax.ppermute(pieces[r], axis, [(i, i ^ r) for i in range(size)])
    return total


def gram_kernel(own_ref, near_ref, far_ref, o_own_ref, o_near_ref, o_far_ref, out_ref):
    others = (own_ref, o_own_ref, near_ref, o_near_ref, far_ref, o_far_ref)
    for tile, other in enumerate(others):
        out_ref[tile] = lax.dot_general(
            own_ref[...],
            other[...],
            (((1,), (1,)), ((), ())),
            precision=EXACT,
            preferred_element_type=F32,
        )


def gram_tiles(*blocks):
    return pl.pallas_call(
        gram_kernel,
        out_shape=jax.ShapeDtypeStruct((6, TILE, TILE), F32),
        compiler_params=vmem(),
        name="gram",
    )(*blocks)


def over_lanes(block, lane):
    return jnp.broadcast_to(block[:, lane : lane + 1], (8, TILE))


def over_rows(block, row):
    return jnp.broadcast_to(block[row : row + 1, :], (8, TILE))


def inverse_root(d):
    root = lax.rsqrt(d)
    return root


def factor_kernel(at_ref, *refs):
    tile_refs = refs[:8]
    out_ref, work, inverse = refs[8:]
    y, c, row0 = at_ref[0], at_ref[1], at_ref[2]
    for n, ref in enumerate(tile_refs):
        shift, other = n % 4, n // 4
        ys, cs = (y + shift) % 4, c ^ other
        a = 2 * ys + cs

        def place(tile, carry, ref=ref, ys=ys, cs=cs, a=a):
            dy, dc = tile // 2, tile % 2
            b = 2 * ((ys + dy) % 4) + (cs ^ dc)

            @pl.when(a <= b)
            def _():
                work[b, pl.ds(pl.multiple_of(a * TILE, TILE), TILE), :] = ref[tile] * 2.0

            @pl.when(a > b)
            def _():
                work[a, pl.ds(pl.multiple_of(b * TILE, TILE), TILE), :] = ref[tile].T * 2.0

            return carry

        lax.fori_loop(0, ref.shape[0], place, 0)

    row_of = lax.broadcasted_iota(jnp.int32, (8, TILE), 0)
    lane_of = lax.broadcasted_iota(jnp.int32, (8, TILE), 1)

    def one_block(j, carry):
        base = j * TILE

        def rows(i):
            return pl.ds(pl.multiple_of(base + 8 * i, 8), 8)

        for above in range(1, 8):

            @pl.when(j == above)
            def _(above=above):
                deep = above * TILE
                mine = work[above, 0:deep, :].T
                for k in range(above, 8):
                    into = slice(deep, deep + TILE)
                    work[k, into, :] = work[k, into, :] - jnp.dot(
                        mine,
                        work[k, 0:deep, :],
                        precision=EXACT,
                        preferred_element_type=F32,
                    )

        tile = [work[j, rows(i), :] for i in range(16)]
        columns = [over_lanes(tile[0], m) for m in range(8)]
        unit = [jnp.where(lane_of == row_of + 8 * i, 1.0, 0.0) for i in range(16)]
        for t in range(16):
            head = tile[t]
            unit_head = unit[t]
            nexts = []
            if t < 15:
                nexts = [over_lanes(tile[t + 1], 8 * (t + 1) + q) for q in range(8)]
            roots, pairs = [], {}
            scale = jnp.zeros((8, TILE), F32)
            for m in range(8):
                root = inverse_root(over_rows(columns[m], m))
                column = columns[m] * root
                for q in range(m + 1, 8):
                    pairs[q, m] = over_rows(columns[m], q) * root
                    columns[q] = columns[q] - column * pairs[q, m]
                masked = jnp.where(row_of > m, column * root, 0.0)
                head = head - masked * over_rows(head, m)
                unit_head = unit_head - masked * over_rows(unit_head, m)
                roots.append(root)
                scale = jnp.where(row_of == m, root, scale)
            head = head * scale
            work[j, rows(t), :] = head
            lines = [over_rows(head, m) for m in range(8)]
            unit_head = unit_head * scale
            inverse[8 * t : 8 * t + 8, :] = unit_head
            unit_lines = [over_rows(unit_head, m) for m in range(8)]
            for i in range(t + 1, 16):
                got = []
                for m in range(8):
                    value = over_lanes(tile[i], 8 * t + m)
                    for q in range(m):
                        value = value - got[q] * pairs[m, q]
                    got.append(value * roots[m])
                for m in range(8):
                    tile[i] = tile[i] - got[m] * lines[m]
                    unit[i] = unit[i] - got[m] * unit_lines[m]
                if i == t + 1:
                    for q in range(8):
                        for m in range(8):
                            nexts[q] = nexts[q] - got[m] * over_rows(got[m], q)
            columns = nexts

        for done in range(7):

            @pl.when(j == done)
            def _(done=done):
                into = slice(done * TILE, (done + 1) * TILE)
                for k in range(done + 1, 8):
                    work[k, into, :] = jnp.dot(
                        inverse[...],
                        work[k, into, :],
                        precision=EXACT,
                        preferred_element_type=F32,
                    )

        return carry

    lax.fori_loop(0, 8, one_block, 0)
    count = out_ref.shape[0]
    row = row0 + lax.broadcasted_iota(jnp.int32, (count, TILE), 0)
    for k in range(8):
        col = k * TILE + lax.broadcasted_iota(jnp.int32, (count, TILE), 1)
        mine = work[k, pl.ds(pl.multiple_of(row0, count), count), :]
        out_ref[:, k * TILE : (k + 1) * TILE] = jnp.where(col >= row, mine, 0.0)


def factored(at, tiles, share):
    return pl.pallas_call(
        factor_kernel,
        in_specs=[pl.BlockSpec(memory_space=pltpu.SMEM)]
        + [pl.BlockSpec(memory_space=pltpu.VMEM)] * len(tiles),
        out_specs=pl.BlockSpec(memory_space=pltpu.VMEM),
        out_shape=jax.ShapeDtypeStruct((share, COLS), F32),
        scratch_shapes=[
            pltpu.VMEM((8, COLS, TILE), F32),
            pltpu.VMEM((TILE, TILE), F32),
        ],
        compiler_params=vmem(),
        name="factor",
    )(at, *tiles)


def from_ahead(array, axis, shift):
    size = lax.axis_size(axis)
    return lax.ppermute(array, axis, [((i + shift) % size, i) for i in range(size)])


def in_line(array, axis):
    lines = array[None]
    for bit in (1, 2, 4):
        other = lax.ppermute(lines, axis, [(i, i ^ bit) for i in range(8)])
        low = lax.axis_index(axis) & bit == 0
        lines = jnp.concatenate([jnp.where(low, lines, other), jnp.where(low, other, lines)])
    return lines


def all_samples(samples):
    lines = jnp.broadcast_to(samples[None, None], (32, 1, samples.shape[0]))
    lines = lax.all_to_all(lines, PLANE, 0, 0, tiled=True)
    return in_line(lines, "z").reshape(8, 32, -1)


def shards(matrix, row_signs, samples):
    rows, cols = matrix.shape
    at_y, at_c = lax.axis_index("y"), lax.axis_index("c")
    at_z, at_x = lax.axis_index("z"), lax.axis_index("x")
    drawn = all_samples(samples)
    first, second = turned(at_z.reshape(1), matrix, row_signs)
    blocks = lax.all_to_all(first.reshape(32, NEAR, rows), PLANE, 0, 0, tiled=True)
    drawn, second = lax.optimization_barrier((drawn, second))
    pieces = [second[0]]
    for s in range(1, 8):
        pieces.append(lax.ppermute(second[s], "z", [(i, i ^ s) for i in range(8)]))
    at = jnp.stack([at_z, jnp.zeros_like(at_z)]).astype(jnp.int32)
    near_signs = sampled_signs(at, drawn.transpose(1, 0, 2).reshape(32, -1))
    at = jnp.stack([lax.axis_index(PLANE), at_z]).astype(jnp.int32)
    far_signs = sampled_signs(at, drawn.reshape(8, -1))
    far_signs, near_signs = lax.optimization_barrier((far_signs, near_signs))
    at = jnp.stack([at_x, at_y, at_c]).astype(jnp.int32)
    ours = far_picked(at, pieces, *far_signs)
    ours = sum_of_pieces([ours[r] for r in range(4)], "x")
    ours = sum_of_pieces([ours[2 * r : 2 * r + 2] for r in range(4)], "y")
    ours = sum_of_pieces([ours[0], ours[1]], "c")
    swap = [(8 * i + j, 8 * j + i) for i in range(8) for j in range(8)]
    others = lax.ppermute(ours, ("z", "y", "c"), swap)
    ours = near_picked(blocks, *near_signs).reshape(32, NEAR, 256)
    arrived = lax.all_to_all(ours, ("x", "z"), 0, 0, tiled=True)
    own = arrived.reshape(4, 8, NEAR, 256).sum(axis=1).reshape(4 * NEAR, 256)
    own = jnp.concatenate([own, others], axis=0)
    near, far = from_ahead(own, "y", 1), from_ahead(own, "y", 2)
    others = [from_ahead(a, "c", 1) for a in (own, near, far)]
    tiles = gram_tiles(own, near, far, *others).reshape(32, 24, TILE)
    share = lax.all_to_all(tiles, ("z", "x"), 0, 0, tiled=True).sum(axis=0)
    whole = jnp.broadcast_to(share[None], (32, 24, TILE))
    whole = lax.all_to_all(whole, ("z", "x"), 0, 0, tiled=True).reshape(6, TILE, TILE)
    lines = [whole, from_ahead(whole, "y", 1)]
    lines += [from_ahead(whole[:4], "y", 2), from_ahead(whole[:4], "y", 3)]
    lines += [from_ahead(a, "c", 1) for a in lines]
    out_rows = COLS // 32
    at = jnp.stack([at_y, at_c, (at_x * 8 + at_z) * out_rows]).astype(jnp.int32)
    return factored(at, lines, out_rows)


def solution(mesh):
    finer = Mesh(mesh.devices.reshape(4, 8, 4, 2), ALL)
    return jax.shard_map(
        shards,
        mesh=finer,
        in_specs=(P(ALL, None), P(ALL), P(ALL)),
        out_specs=P(("x", "z"), None),
        check_vma=False,
    )
```

```python
import functools

import jax
import jax.numpy as jnp
from jax import lax
from jax.experimental import pallas as pl
from jax.experimental.pallas import tpu as pltpu
from jax.sharding import Mesh
from jax.sharding import PartitionSpec as P

ALL = ("x", "z", "y", "c")
PLANE = ("y", "c", "x")
EXACT = lax.Precision.HIGHEST
F32 = jnp.float32
BF16 = jnp.bfloat16
COLS = 1024
TILE = 128
NEAR = 24
FAR = 32
STEPS = 4


def vmem(limit=100):
    return pltpu.CompilerParams(vmem_limit_bytes=limit * 1024 * 1024 // 2)


def turn_kernel(z_ref, sign_ref, in_ref, near_ref, far_ref):
    del z_ref
    for t in range(in_ref.shape[0] // TILE):
        rows = slice(t * TILE, (t + 1) * TILE)
        lines = in_ref[rows, :].T * sign_ref[t : t + 1, :].astype(F32)
        near_ref[:, rows] = lines[: 4 * NEAR, :]
        far_ref[0, :, rows] = lines[4 * NEAR :, :]


def turned(z_index, matrix, row_signs):
    rows, cols = matrix.shape
    signs = row_signs.reshape(rows // TILE, TILE)
    return pl.pallas_call(
        turn_kernel,
        grid_spec=pltpu.PrefetchScalarGridSpec(
            num_scalar_prefetch=1,
            grid=(cols // TILE,),
            in_specs=[
                pl.BlockSpec(signs.shape, lambda i, z: (0, 0)),
                pl.BlockSpec((rows, TILE), lambda i, z: (0, i)),
            ],
            out_specs=[
                pl.BlockSpec((4 * NEAR, rows), lambda i, z: (i, 0)),
                pl.BlockSpec((1, FAR, rows), lambda i, z: (i ^ z[0], 0, 0)),
            ],
        ),
        out_shape=[
            jax.ShapeDtypeStruct((32 * NEAR, rows), F32),
            jax.ShapeDtypeStruct((8, FAR, rows), F32),
        ],
        compiler_params=vmem(),
        name="turn",
    )(z_index, signs, matrix)


def odd_ones(bits):
    for shift in (4, 2, 1):
        bits = bits ^ (bits >> shift)
    return bits & 1


def signs_kernel(at_ref, sample_ref, low_ref, high_ref):
    block = pl.program_id(0)
    count = low_ref.shape[2]
    within = sample_ref[pl.ds(block, 1), :] & 2047
    for lane in range(0, count, 256):
        lanes = slice(lane, lane + 256)
        wl = lax.broadcasted_iota(jnp.int32, (256, 256), 0)
        low = odd_ones(wl & (within[:, lanes] & 255))
        low_ref[0, :, lanes] = (1 - 2 * low).astype(F32).astype(BF16)
    wh = lax.broadcasted_iota(jnp.int32, (8, count), 0)
    lane = lax.broadcasted_iota(jnp.int32, (8, count), 1)
    odd = odd_ones(wh & (within >> 8)) ^ odd_ones((lane >> 5) & at_ref[0])
    odd = odd ^ odd_ones(block & at_ref[1])
    high_ref[0] = (1 - 2 * odd).astype(F32) * (2.0**-7)


def sampled_signs(at, samples):
    blocks, count = samples.shape
    return pl.pallas_call(
        signs_kernel,
        grid=(blocks,),
        in_specs=[
            pl.BlockSpec(memory_space=pltpu.SMEM),
            pl.BlockSpec((blocks, count), lambda i: (0, 0)),
        ],
        out_specs=[
            pl.BlockSpec((1, 256, count), lambda i: (i, 0, 0)),
            pl.BlockSpec((1, 8, count), lambda i: (i, 0, 0)),
        ],
        out_shape=[
            jax.ShapeDtypeStruct((blocks, 256, count), BF16),
            jax.ShapeDtypeStruct((blocks, 8, count), F32),
        ],
        compiler_params=vmem(),
        name="signs",
    )(at, samples)


def butterflies(values):
    span = 1
    while span < len(values):
        new = list(values)
        for i in range(len(values)):
            if not i & span:
                new[i] = values[i] + values[i + span]
                new[i + span] = values[i] - values[i + span]
        values = new
        span *= 2
    return values


def mix_blocks(step, read, count, cols, parts_ref):
    pieces = [(wh, col) for wh in range(2) for col in range(0, cols, 8)]
    for n in range(0, len(pieces), 2):
        for lane in range(0, 256, TILE):
            both = []
            for wh, col in pieces[n : n + 2]:
                first = 256 * wh + lane
                lanes = slice(first, first + TILE)
                both.append([read(p, slice(col, col + 8), lanes) for p in range(count)])
            values = [jnp.concatenate(pair, axis=0) for pair in zip(*both)]
            for p, rest in enumerate(butterflies(values)):
                for part in range(2):
                    piece = rest.astype(BF16)
                    parts_ref[p, part, step, 8 * n : 8 * n + 16, lane : lane + TILE] = piece
                    if part < 1:
                        rest = rest - piece.astype(F32)


def pick_rows(lines, low, high, cols):
    got = jnp.dot(lines, low, preferred_element_type=F32)
    size = 8 * cols
    got = got[:size] + got[size:]
    total = got[:cols] * high[0:1]
    for wh in range(1, 8):
        total = total + got[cols * wh : cols * (wh + 1)] * high[wh : wh + 1]
    return total


def near_kernel(in_ref, low_ref, high_ref, out_ref, parts_ref, rows_ref):
    step = pl.program_id(0)

    @pl.when(step < STEPS)
    def _():
        read = lambda p, cols, lanes: in_ref[p, cols, lanes]
        mix_blocks(step, read, 32, NEAR, parts_ref)

    @pl.when(step >= STEPS)
    def _():
        def one(n, carry):
            lines = parts_ref[(step - STEPS) * 8 + n].reshape(16 * NEAR, 256)
            rows_ref[n] = pick_rows(lines, low_ref[n], high_ref[n], NEAR)
            return carry

        lax.fori_loop(0, 8, one, 0, unroll=2)
        group = lax.broadcasted_iota(jnp.int32, (NEAR, TILE), 1) >> 5
        for z in range(8):
            lanes = slice(TILE * (z // 4), TILE * (z // 4) + TILE)
            for half in range(2):
                total = jnp.zeros((NEAR, TILE), F32)
                for n in range(4):
                    block = rows_ref[4 * half + n, :, lanes]
                    block = pltpu.roll(block, (32 * n - 32 * (z % 4)) % TILE, 1)
                    total = jnp.where(group == n, block, total)
                out_ref[0, z, :, TILE * half : TILE * half + TILE] = total


def late(i):
    return jnp.maximum(i - STEPS, 0)


def early(i):
    return jnp.minimum(i, STEPS - 1)


def near_picked(blocks, low, high):
    wide = blocks.shape[2] // STEPS
    return pl.pallas_call(
        near_kernel,
        grid=(2 * STEPS,),
        in_specs=[
            pl.BlockSpec((32, NEAR, wide), lambda i: (0, 0, early(i))),
            pl.BlockSpec((8, 256, 256), lambda i: (late(i), 0, 0)),
            pl.BlockSpec((8, 8, 256), lambda i: (late(i), 0, 0)),
        ],
        out_specs=pl.BlockSpec((1, 8, NEAR, 256), lambda i: (late(i), 0, 0, 0)),
        out_shape=jax.ShapeDtypeStruct((4, 8, NEAR, 256), F32),
        scratch_shapes=[
            pltpu.VMEM((32, 2, STEPS, 2 * NEAR, 256), BF16),
            pltpu.VMEM((8, NEAR, 256), F32),
        ],
        compiler_params=vmem(),
        name="near",
    )(blocks, low, high)


def far_kernel(at_ref, *refs):
    in_refs = refs[:8]
    low_ref, high_ref, out_ref, parts_ref = refs[8:]
    step = pl.program_id(0)

    @pl.when(step < STEPS)
    def _():
        read = lambda p, cols, lanes: in_refs[p][cols, lanes]
        mix_blocks(step, read, 8, FAR, parts_ref)

    @pl.when(step >= STEPS)
    def _():
        def one(n, carry):
            lines = parts_ref[(step - STEPS) * 2 + n].reshape(16 * FAR, 256)
            for q in range(4):
                lanes = slice(256 * q, 256 * q + 256)
                got = pick_rows(lines, low_ref[n, :, lanes], high_ref[n, :, lanes], FAR)
                out_ref[q ^ at_ref[0], n ^ at_ref[2]] = got
            return carry

        lax.fori_loop(0, 2, one, 0)


def far_picked(at, pieces, low, high):
    wide = pieces[0].shape[1] // STEPS
    return pl.pallas_call(
        far_kernel,
        grid_spec=pltpu.PrefetchScalarGridSpec(
            num_scalar_prefetch=1,
            grid=(2 * STEPS,),
            in_specs=[pl.BlockSpec((FAR, wide), lambda i, at: (0, early(i)))] * 8
            + [
                pl.BlockSpec((2, 256, 1024), lambda i, at: (late(i), 0, 0)),
                pl.BlockSpec((2, 8, 1024), lambda i, at: (late(i), 0, 0)),
            ],
            out_specs=pl.BlockSpec(
                (4, 2, FAR, 256), lambda i, at: (0, late(i) ^ at[1], 0, 0)
            ),
            scratch_shapes=[pltpu.VMEM((8, 2, STEPS, 2 * FAR, 256), BF16)],
        ),
        out_shape=jax.ShapeDtypeStruct((4, 8, FAR, 256), F32),
        compiler_params=vmem(),
        name="far",
    )(at, *pieces, low, high)


def sum_of_pieces(pieces, axis):
    total = pieces[0]
    size = len(pieces)
    for r in range(1, size):
        total = total + lax.ppermute(pieces[r], axis, [(i, i ^ r) for i in range(size)])
    return total


def gram_kernel(own_ref, near_ref, far_ref, o_own_ref, o_near_ref, o_far_ref, out_ref):
    others = (own_ref, o_own_ref, near_ref, o_near_ref, far_ref, o_far_ref)
    for tile, other in enumerate(others):
        out_ref[tile] = lax.dot_general(
            own_ref[...],
            other[...],
            (((1,), (1,)), ((), ())),
            precision=EXACT,
            preferred_element_type=F32,
        )


def gram_tiles(*blocks):
    return pl.pallas_call(
        gram_kernel,
        out_shape=jax.ShapeDtypeStruct((6, TILE, TILE), F32),
        compiler_params=vmem(),
        name="gram",
    )(*blocks)


def over_lanes(block, lane):
    return jnp.broadcast_to(block[:, lane : lane + 1], (8, TILE))


def over_rows(block, row):
    return jnp.broadcast_to(block[row : row + 1, :], (8, TILE))


def inverse_root(d):
    root = lax.rsqrt(d)
    return root


def factor_kernel(at_ref, *refs):
    tile_refs = refs[:8]
    out_ref, work, inverse = refs[8:]
    y, c, row0 = at_ref[0], at_ref[1], at_ref[2]
    for n, ref in enumerate(tile_refs):
        shift, other = n % 4, n // 4
        ys, cs = (y + shift) % 4, c ^ other
        a = 2 * ys + cs

        def place(tile, carry, ref=ref, ys=ys, cs=cs, a=a):
            dy, dc = tile // 2, tile % 2
            b = 2 * ((ys + dy) % 4) + (cs ^ dc)

            @pl.when(a <= b)
            def _():
                work[b, pl.ds(pl.multiple_of(a * TILE, TILE), TILE), :] = ref[tile] * 2.0

            @pl.when(a > b)
            def _():
                work[a, pl.ds(pl.multiple_of(b * TILE, TILE), TILE), :] = ref[tile].T * 2.0

            return carry

        lax.fori_loop(0, ref.shape[0], place, 0)

    row_of = lax.broadcasted_iota(jnp.int32, (8, TILE), 0)
    lane_of = lax.broadcasted_iota(jnp.int32, (8, TILE), 1)

    def one_block(j, carry):
        base = j * TILE

        def rows(i):
            return pl.ds(pl.multiple_of(base + 8 * i, 8), 8)

        for above in range(1, 8):

            @pl.when(j == above)
            def _(above=above):
                deep = above * TILE
                mine = work[above, 0:deep, :].T
                for k in range(above, 8):
                    into = slice(deep, deep + TILE)
                    work[k, into, :] = work[k, into, :] - jnp.dot(
                        mine,
                        work[k, 0:deep, :],
                        precision=EXACT,
                        preferred_element_type=F32,
                    )

        tile = [work[j, rows(i), :] for i in range(16)]
        columns = [over_lanes(tile[0], m) for m in range(8)]
        unit = [jnp.where(lane_of == row_of + 8 * i, 1.0, 0.0) for i in range(16)]
        for t in range(16):
            head = tile[t]
            unit_head = unit[t]
            nexts = []
            if t < 15:
                nexts = [over_lanes(tile[t + 1], 8 * (t + 1) + q) for q in range(8)]
            roots, pairs = [], {}
            scale = jnp.zeros((8, TILE), F32)
            for m in range(8):
                root = inverse_root(over_rows(columns[m], m))
                column = columns[m] * root
                for q in range(m + 1, 8):
                    pairs[q, m] = over_rows(columns[m], q) * root
                    columns[q] = columns[q] - column * pairs[q, m]
                masked = jnp.where(row_of > m, column * root, 0.0)
                head = head - masked * over_rows(head, m)
                unit_head = unit_head - masked * over_rows(unit_head, m)
                roots.append(root)
                scale = jnp.where(row_of == m, root, scale)
            head = head * scale
            work[j, rows(t), :] = head
            lines = [over_rows(head, m) for m in range(8)]
            unit_head = unit_head * scale
            inverse[8 * t : 8 * t + 8, :] = unit_head
            unit_lines = [over_rows(unit_head, m) for m in range(8)]
            for i in range(t + 1, 16):
                got = []
                for m in range(8):
                    value = over_lanes(tile[i], 8 * t + m)
                    for q in range(m):
                        value = value - got[q] * pairs[m, q]
                    got.append(value * roots[m])
                for m in range(8):
                    tile[i] = tile[i] - got[m] * lines[m]
                    unit[i] = unit[i] - got[m] * unit_lines[m]
                if i == t + 1:
                    for q in range(8):
                        for m in range(8):
                            nexts[q] = nexts[q] - got[m] * over_rows(got[m], q)
            columns = nexts

        for done in range(7):

            @pl.when(j == done)
            def _(done=done):
                into = slice(done * TILE, (done + 1) * TILE)
                for k in range(done + 1, 8):
                    work[k, into, :] = jnp.dot(
                        inverse[...],
                        work[k, into, :],
                        precision=EXACT,
                        preferred_element_type=F32,
                    )

        return carry

    lax.fori_loop(0, 8, one_block, 0)
    count = out_ref.shape[0]
    row = row0 + lax.broadcasted_iota(jnp.int32, (count, TILE), 0)
    for k in range(8):
        col = k * TILE + lax.broadcasted_iota(jnp.int32, (count, TILE), 1)
        mine = work[k, pl.ds(pl.multiple_of(row0, count), count), :]
        out_ref[:, k * TILE : (k + 1) * TILE] = jnp.where(col >= row, mine, 0.0)


def factored(at, tiles, share):
    return pl.pallas_call(
        factor_kernel,
        in_specs=[pl.BlockSpec(memory_space=pltpu.SMEM)]
        + [pl.BlockSpec(memory_space=pltpu.VMEM)] * len(tiles),
        out_specs=pl.BlockSpec(memory_space=pltpu.VMEM),
        out_shape=jax.ShapeDtypeStruct((share, COLS), F32),
        scratch_shapes=[
            pltpu.VMEM((8, COLS, TILE), F32),
            pltpu.VMEM((TILE, TILE), F32),
        ],
        compiler_params=vmem(),
        name="factor",
    )(at, *tiles)


def from_ahead(array, axis, shift):
    size = lax.axis_size(axis)
    return lax.ppermute(array, axis, [((i + shift) % size, i) for i in range(size)])


def in_line(array, axis):
    lines = array[None]
    for bit in (1, 2, 4):
        other = lax.ppermute(lines, axis, [(i, i ^ bit) for i in range(8)])
        low = lax.axis_index(axis) & bit == 0
        lines = jnp.concatenate([jnp.where(low, lines, other), jnp.where(low, other, lines)])
    return lines


def all_samples(samples):
    lines = jnp.broadcast_to(samples[None, None], (32, 1, samples.shape[0]))
    lines = lax.all_to_all(lines, PLANE, 0, 0, tiled=True)
    return in_line(lines, "z").reshape(8, 32, -1)


def shards(matrix, row_signs, samples):
    rows, cols = matrix.shape
    at_y, at_c = lax.axis_index("y"), lax.axis_index("c")
    at_z, at_x = lax.axis_index("z"), lax.axis_index("x")
    drawn = all_samples(samples)
    first, second = turned(at_z.reshape(1), matrix, row_signs)
    blocks = lax.all_to_all(first.reshape(32, NEAR, rows), PLANE, 0, 0, tiled=True)
    drawn, second = lax.optimization_barrier((drawn, second))
    pieces = [second[0]]
    for s in range(1, 8):
        pieces.append(lax.ppermute(second[s], "z", [(i, i ^ s) for i in range(8)]))
    at = jnp.stack([at_z, jnp.zeros_like(at_z)]).astype(jnp.int32)
    near_signs = sampled_signs(at, drawn.transpose(1, 0, 2).reshape(32, -1))
    at = jnp.stack([lax.axis_index(PLANE), at_z]).astype(jnp.int32)
    far_signs = sampled_signs(at, drawn.reshape(8, -1))
    far_signs, near_signs = lax.optimization_barrier((far_signs, near_signs))
    at = jnp.stack([at_x, at_y, at_c]).astype(jnp.int32)
    ours = far_picked(at, pieces, *far_signs)
    ours = sum_of_pieces([ours[r] for r in range(4)], "x")
    ours = sum_of_pieces([ours[2 * r : 2 * r + 2] for r in range(4)], "y")
    ours = sum_of_pieces([ours[0], ours[1]], "c")
    swap = [(8 * i + j, 8 * j + i) for i in range(8) for j in range(8)]
    others = lax.ppermute(ours, ("z", "y", "c"), swap)
    ours = near_picked(blocks, *near_signs).reshape(32, NEAR, 256)
    arrived = lax.all_to_all(ours, ("x", "z"), 0, 0, tiled=True)
    own = arrived.reshape(4, 8, NEAR, 256).sum(axis=1).reshape(4 * NEAR, 256)
    own = jnp.concatenate([own, others], axis=0)
    near, far = from_ahead(own, "y", 1), from_ahead(own, "y", 2)
    others = [from_ahead(a, "c", 1) for a in (own, near, far)]
    tiles = gram_tiles(own, near, far, *others).reshape(32, 24, TILE)
    share = lax.all_to_all(tiles, ("z", "x"), 0, 0, tiled=True).sum(axis=0)
    whole = jnp.broadcast_to(share[None], (32, 24, TILE))
    whole = lax.all_to_all(whole, ("z", "x"), 0, 0, tiled=True).reshape(6, TILE, TILE)
    lines = [whole, from_ahead(whole, "y", 1)]
    lines += [from_ahead(whole[:4], "y", 2), from_ahead(whole[:4], "y", 3)]
    lines += [from_ahead(a, "c", 1) for a in lines]
    out_rows = COLS // 32
    at = jnp.stack([at_y, at_c, (at_x * 8 + at_z) * out_rows]).astype(jnp.int32)
    return factored(at, lines, out_rows)


def solution(mesh):
    finer = Mesh(mesh.devices.reshape(4, 8, 4, 2), ALL)
    return jax.shard_map(
        shards,
        mesh=finer,
        in_specs=(P(ALL, None), P(ALL), P(ALL)),
        out_specs=P(("x", "z"), None),
        check_vma=False,
    )
```
